128 devices in a mesh: gy: 8 (over y, x_hi), gx: 4 (over z), gz: 4 (over x_lo, core).
Axes of the slice: x: 4 (x_hi: 2, x_lo: 2; x = x_hi * 2 + x_lo), y: 4, z: 4, core: 2. Of those that a mesh axis runs over, the one named last changes fastest.
Arguments:
- potential_warmth: float32 [32, 1024, 512], P('gz', 'gy', 'gx'), may hold values from -6 to 6
- saltiness_anomaly: float32 [32, 1024, 512], P('gz', 'gy', 'gx'), may hold values from -6 to 6
- squared_brunt_vaisala: float32 [32, 1024, 512], P('gz', 'gy', 'gx'), may hold values from 0.5 to 2
- cross_density_mixing: float32 [32, 1024, 512], P('gz', 'gy', 'gx'), may hold values from 0.1 to 10
- along_neutral_mixing: float32 [32, 1024, 512], P('gz', 'gy', 'gx'), may hold values from 0.04 to 0.2
- layer_depth_mixing: float32 [32, 1024, 512], P('gz', 'gy', 'gx'), may hold values from 0.04 to 0.2
- seawater_profile_flag: int32 [1024, 512], P('gy', 'gx'), may hold values 0 or 1
- submerged_layer_total: int32 [1024, 512], P('gy', 'gx'), may hold values from 1 to 32
Outputs:
- temperature_new: float32 [32, 1024, 512], P('gz', 'gy', 'gx')
- salinity_new: float32 [32, 1024, 512], P('gz', 'gy', 'gx')
The draws below stay inside these ranges and needn't reach their ends.
All inputs are finite; a program needn't handle non-finite values. No bound on the sum of `seawater_profile_flag` on one device may be relied on, other than what follows from the above.
Results may differ from the reference program's by a relative error of at most 0.00002.
Values sent between devices are 32-bit elements; how exact they have to be, the bound alone decides.
No kernel may reach another device: no remote copies, remote signals or barrier semaphores. Data moves between devices by JAX's collectives and lax.ppermute only.
A program may use at most 128 MiB of HBM per device.

```python
import math
import jax
import jax.numpy as jnp
from jax import lax

EAST_WEST_SPAN = 512
NORTH_SOUTH_SPAN = 1024
DEPTH_STRATA = 32


def place_ends(drawn, key, least, largest):
    dims = drawn.shape
    index_at = [jax.random.randint(jax.random.fold_in(key, axis), (), 0, dims[axis]) for axis in range(len(dims))]
    drawn = drawn.at[tuple(index_at)].set(least)
    longest = dims.index(max(dims))
    index_at[longest] = (index_at[longest] + 1) % dims[longest]
    return drawn.at[tuple(index_at)].set(largest)


def block_levels(stream_key, shape, pieces, least, high):
    def one(position, parts):
        steps = jax.random.uniform(jax.random.fold_in(jax.random.fold_in(stream_key, 6), position), (parts,), jnp.float32, least / len(pieces), high / len(pieces))
        return jnp.repeat(jnp.exp(steps), shape[position] // parts).reshape((-1,) + (1,) * (len(shape) - position - 1))

    factor_of = one(*pieces[0])
    for cut in pieces[1:]:
        factor_of = factor_of * one(*cut)
    return factor_of


def gaussian(rng, shape, scale, reach, shards=(), held_as=jnp.bfloat16):
    entries = scale * jax.random.normal(rng, shape, jnp.float32)
    if shards:
        entries = entries * block_levels(rng, shape, shards, -0.22, 0.18)
    return jnp.clip(entries, -reach, reach).astype(held_as)


def setup_inputs(seed: int = 0) -> dict:
    streams_of = jax.random.split(jax.random.key(seed), 9)
    potential_warmth = gaussian(streams_of[0], (DEPTH_STRATA, NORTH_SOUTH_SPAN, EAST_WEST_SPAN), 1.0, 6.0, ((0, 4), (1, 8), (2, 4)), jnp.float32)
    saltiness_anomaly = gaussian(streams_of[1], (DEPTH_STRATA, NORTH_SOUTH_SPAN, EAST_WEST_SPAN), 1.0, 6.0, ((0, 4), (1, 8), (2, 4)), jnp.float32)
    squared_brunt_vaisala = jnp.clip(jnp.exp(math.log(2.0) - 1.3862944 * jax.random.uniform(streams_of[2], (DEPTH_STRATA, NORTH_SOUTH_SPAN, EAST_WEST_SPAN), jnp.float32) ** block_levels(streams_of[2], (DEPTH_STRATA, NORTH_SOUTH_SPAN, EAST_WEST_SPAN), ((0, 4), (1, 8), (2, 4)), -0.2, 0.2)), 0.5, 2.0)
    cross_density_mixing = jnp.clip(jnp.exp(math.log(10.0) - 4.6051702 * jax.random.uniform(streams_of[3], (DEPTH_STRATA, NORTH_SOUTH_SPAN, EAST_WEST_SPAN), jnp.float32) ** block_levels(streams_of[3], (DEPTH_STRATA, NORTH_SOUTH_SPAN, EAST_WEST_SPAN), ((0, 4), (1, 8), (2, 4)), -0.2, 0.2)), 0.1, 10.0)
    along_neutral_mixing = jnp.clip(jnp.exp(math.log(0.2) - 1.609438 * jax.random.uniform(streams_of[4], (DEPTH_STRATA, NORTH_SOUTH_SPAN, EAST_WEST_SPAN), jnp.float32) ** block_levels(streams_of[4], (DEPTH_STRATA, NORTH_SOUTH_SPAN, EAST_WEST_SPAN), ((0, 4), (1, 8), (2, 4)), -0.2, 0.2)), 0.04, 0.2)
    layer_depth_mixing = jnp.clip(jnp.exp(math.log(0.2) - 1.609438 * jax.random.uniform(streams_of[5], (DEPTH_STRATA, NORTH_SOUTH_SPAN, EAST_WEST_SPAN), jnp.float32) ** block_levels(streams_of[5], (DEPTH_STRATA, NORTH_SOUTH_SPAN, EAST_WEST_SPAN), ((0, 4), (1, 8), (2, 4)), -0.2, 0.2)), 0.04, 0.2)
    seawater_profile_flag = place_ends((jax.random.randint(streams_of[6], (NORTH_SOUTH_SPAN, EAST_WEST_SPAN), 0, 5) < 4).astype(jnp.int32), jax.random.fold_in(streams_of[6], 1), 0, 1)
    submerged_layer_total = place_ends(jax.random.randint(streams_of[7], (NORTH_SOUTH_SPAN, EAST_WEST_SPAN), 1, DEPTH_STRATA + 1), jax.random.fold_in(streams_of[7], 1), 1, DEPTH_STRATA).astype(jnp.int32)
    return dict(potential_warmth=potential_warmth, saltiness_anomaly=saltiness_anomaly, squared_brunt_vaisala=squared_brunt_vaisala, cross_density_mixing=cross_density_mixing, along_neutral_mixing=along_neutral_mixing, layer_depth_mixing=layer_depth_mixing, seawater_profile_flag=seawater_profile_flag, submerged_layer_total=submerged_layer_total)


step_dt = 1.0


def explicit_part(extended, cross_density_mixing):
    tracer = extended[0:2]
    density_lift_array = extended[2]
    stratum = extended[3]
    seawater_volume_flag = extended[4]
    redi_coef = extended[5]
    bolus_coef = extended[6]
    wet_x = seawater_volume_flag[:, :, 1:] * seawater_volume_flag[:, :, :-1]
    grad_bx = (density_lift_array[:, :, 1:] - density_lift_array[:, :, :-1]) * wet_x
    slope_x = -grad_bx / (0.5 * (stratum[:, :, 1:] + stratum[:, :, :-1]) + jnp.abs(grad_bx) + 1.0 - wet_x)
    diff_x = (tracer[..., 1:] - tracer[..., :-1]) * wet_x
    wet_y = seawater_volume_flag[:, 1:, :] * seawater_volume_flag[:, :-1, :]
    grad_by = (density_lift_array[:, 1:, :] - density_lift_array[:, :-1, :]) * wet_y
    slope_y = -grad_by / (0.5 * (stratum[:, 1:, :] + stratum[:, :-1, :]) + jnp.abs(grad_by) + 1.0 - wet_y)
    diff_y = (tracer[:, :, 1:, :] - tracer[:, :, :-1, :]) * wet_y
    wet_z = seawater_volume_flag[1:] * seawater_volume_flag[:-1]
    diff_z = (tracer[:, 1:] - tracer[:, :-1]) * wet_z
    centre_z = 0.5 * (diff_z[:, 1:] + diff_z[:, :-1])
    redi_x = 0.5 * (redi_coef[1:-1, 1:-1, 1:] + redi_coef[1:-1, 1:-1, :-1])
    bolus_x = 0.5 * (bolus_coef[1:-1, 1:-1, 1:] + bolus_coef[1:-1, 1:-1, :-1])
    flux_x = -(redi_x * diff_x[:, 1:-1, 1:-1, :] + (redi_x - bolus_x) * slope_x[1:-1, 1:-1, :] * 0.5 * (centre_z[:, :, 1:-1, 1:] + centre_z[:, :, 1:-1, :-1]))
    redi_y = 0.5 * (redi_coef[1:-1, 1:, 1:-1] + redi_coef[1:-1, :-1, 1:-1])
    bolus_y = 0.5 * (bolus_coef[1:-1, 1:, 1:-1] + bolus_coef[1:-1, :-1, 1:-1])
    flux_y = -(redi_y * diff_y[:, 1:-1, :, 1:-1] + (redi_y - bolus_y) * slope_y[1:-1, :, 1:-1] * 0.5 * (centre_z[:, :, 1:, 1:-1] + centre_z[:, :, :-1, 1:-1]))
    slope_cx = 0.5 * (slope_x[:, 1:-1, 1:] + slope_x[:, 1:-1, :-1])
    grad_cx = 0.5 * (diff_x[:, :, 1:-1, 1:] + diff_x[:, :, 1:-1, :-1])
    slope_cy = 0.5 * (slope_y[:, 1:, 1:-1] + slope_y[:, :-1, 1:-1])
    grad_cy = 0.5 * (diff_y[:, :, 1:, 1:-1] + diff_y[:, :, :-1, 1:-1])
    cross = slope_cx * grad_cx + slope_cy * grad_cy
    total_coef = (redi_coef + bolus_coef)[:, 1:-1, 1:-1]
    flux_z = -0.5 * (total_coef[1:] * cross[:, 1:] + total_coef[:-1] * cross[:, :-1]) * wet_z[:, 1:-1, 1:-1]
    tendency = -(flux_x[..., 1:] - flux_x[..., :-1]) - (flux_y[:, :, 1:, :] - flux_y[:, :, :-1, :]) - (flux_z[:, 1:] - flux_z[:, :-1])
    inner_wet = seawater_volume_flag[1:-1, 1:-1, 1:-1]
    fresh = (tracer[:, 1:-1, 1:-1, 1:-1] + step_dt * tendency) * inner_wet
    square_slope = slope_cx * slope_cx + slope_cy * slope_cy
    couple = (cross_density_mixing + 0.5 * (redi_coef[1:-1, 1:-1, 1:-1] * square_slope[1:-1] + redi_coef[2:, 1:-1, 1:-1] * square_slope[2:])) * wet_z[1:, 1:-1, 1:-1]
    return fresh, couple


def solve_columns(couple, fresh):
    lower = -step_dt * jnp.concatenate([jnp.zeros_like(couple[:1]), couple[:-1]], axis=0)
    upper = -step_dt * couple
    middle = 1.0 - lower - upper
    right = jnp.moveaxis(fresh, 1, 0)

    def forward(carry, items):
        prev_c, prev_d = carry
        low, mid, upp, rhs = items
        denom = mid - low * prev_c
        next_c = upp / denom
        next_d = (rhs - low * prev_d) / denom
        return (next_c, next_d), (next_c, next_d)

    start = (jnp.zeros(couple.shape[1:], jnp.float32), jnp.zeros(right.shape[1:], jnp.float32))
    _, (coef_c, coef_d) = lax.scan(forward, start, (lower, middle, upper, right))

    def backward(later, items):
        cur_c, cur_d = items
        value = cur_d - cur_c * later
        return value, value

    _, values = lax.scan(backward, jnp.zeros(right.shape[1:], jnp.float32), (coef_c, coef_d), reverse=True)
    return jnp.moveaxis(values, 0, 1)


def reference(potential_warmth, saltiness_anomaly, squared_brunt_vaisala, cross_density_mixing, along_neutral_mixing, layer_depth_mixing, seawater_profile_flag, submerged_layer_total):
    levels = jnp.arange(DEPTH_STRATA, dtype=jnp.int32)[:, None, None]
    seawater_volume_flag = ((seawater_profile_flag[None] == 1) & (levels < submerged_layer_total[None])).astype(jnp.float32)
    density_lift_array = jnp.cumsum(squared_brunt_vaisala, axis=0)
    joined_solutes = jnp.stack([potential_warmth, saltiness_anomaly, density_lift_array, squared_brunt_vaisala, seawater_volume_flag, along_neutral_mixing, layer_depth_mixing])
    joined_solutes = jnp.pad(joined_solutes, ((0, 0), (0, 0), (0, 0), (1, 1)), mode="wrap")
    extended = jnp.pad(joined_solutes, ((0, 0), (1, 1), (1, 1), (0, 0)))
    fresh, couple = explicit_part(extended, cross_density_mixing)
    solved = solve_columns(couple, fresh)
    return solved[0], solved[1]
```

```python
import functools

import jax
import jax.numpy as jnp
from jax import lax
from jax.experimental import pallas as pl
from jax.experimental.pallas import tpu as pltpu
from jax.sharding import PartitionSpec as P

F32 = jnp.float32
LV = 16
HB = 8
RW = 64
HW = 72
PR = 80
LN = 128

VM = pl.BlockSpec(memory_space=pltpu.VMEM)
HM = pl.BlockSpec(memory_space=pltpu.HBM)


def place():
    g = lax.axis_index("gz")
    return lax.div(g, 2), lax.rem(g, 2)


def call(body, outs, in_specs, scratch=(), out_specs=None, aliases=None, name=None):
    return pl.pallas_call(
        body,
        out_shape=[jax.ShapeDtypeStruct(s, d) for s, d in outs],
        in_specs=in_specs,
        out_specs=out_specs or [VM] * len(outs),
        scratch_shapes=list(scratch),
        input_output_aliases=aliases or {},
        compiler_params=pltpu.CompilerParams(vmem_limit_bytes=24 * 2**20),
        name=name,
    )


def k0(t, s, n, ki, kg, cd, swap, own, al, be, sem):
    xl, c = place()
    fields = (n, t, s, ki, kg, cd)
    slots = (2, 0, 1, 3, 4, 5)
    sib = pl.multiple_of(56 * (1 - c), 8)
    mine = pl.multiple_of(56 * c, 8)
    copies = []
    for i, (f, q) in enumerate(zip(fields, slots)):
        copies.append(pltpu.make_async_copy(f.at[:, pl.ds(sib, HW), :], swap.at[q], sem.at[2 * i]))
        copies.append(pltpu.make_async_copy(f.at[:, pl.ds(mine, HW), :], own.at[q], sem.at[2 * i + 1]))
    for cp in copies:
        cp.start()
    e = HB - 1 - (HB - 1) * xl
    for i, q in enumerate(slots):
        copies[2 * i].wait()
        copies[2 * i + 1].wait()
        for src, dst in ((swap, al), (own, be)):
            if q == 2:
                total = src[2, 0]
                for j in range(1, HB):
                    total = total + src[2, j]
                dst[2] = total
            elif q < 2:
                dst[q] = src[q, e]


def k1(own, rec, al, be, prof, subm, fa, cs, dep, edge, mr, ml, yy, nr):
    xl, c = place()
    xf = xl.astype(F32)
    r0 = pl.multiple_of(8 * (1 - c), 8)
    rows = pl.ds(r0, HW)
    src0 = pl.ds(pl.multiple_of(56 * c, 8), HW)
    dep[...] = jnp.zeros_like(dep)
    d = jnp.where(prof[src0, :] == 1, subm[src0, :], 0)
    dep[rows, :] = d
    cs[LV * xl] = jnp.zeros((PR, LN), F32)
    base = jnp.where(c == xl, 0, HB)
    for src, b0 in ((own, base), (rec, HB - base)):
        for j in range(HB):
            l = b0 + j + xl * (HB - 1 - 2 * j)
            k = l + xl * (31 - 2 * l)
            fa[0, l, rows, :] = src[0, j]
            fa[1, l, rows, :] = src[1, j]
            n = src[2, j]
            nr[l, rows, :] = n
            fa[4, l, rows, :] = jnp.where(d > k, n, 0.0)
            ki = src[3, j]
            fa[6, l, rows, :] = ki
            fa[7, l, rows, :] = ki - src[4, j]
            cs[l + 1 - xl, rows, :] = src[5, j]
    use_al = (c + xl) == 1
    for i in range(3):
        rr = pl.ds(pl.multiple_of(r0 + 24 * i, 8), 24)
        mr_ = pl.ds(24 * i, 24)
        total = al[2, mr_, :] + be[2, mr_, :]
        for l in range(LV):
            total = total + nr[l, rr, :]
        acc = -xf * total
        dd = dep[rr, :]
        t16 = jnp.where(use_al, al[0, mr_, :], be[0, mr_, :])
        s16 = jnp.where(use_al, al[1, mr_, :], be[1, mr_, :])
        pt = jnp.zeros((24, LN), F32)
        ps = pt
        tc = fa[0, 0, rr, :]
        sc = fa[1, 0, rr, :]
        for l in range(LV):
            n = nr[l, rr, :]
            fa[5, l, rr, :] = acc + (1.0 - xf) * n
            acc = acc + n
            tn = fa[0, l + 1, rr, :] if l < LV - 1 else t16
            sn = fa[1, l + 1, rr, :] if l < LV - 1 else s16
            ok = dd > (l + 1 + xl * (30 - 2 * l))
            zt = jnp.where(ok, tn - tc, 0.0)
            zs = jnp.where(ok, sn - sc, 0.0)
            fa[2, l, rr, :] = pt + zt
            fa[3, l, rr, :] = ps + zs
            pt, ps, tc, sc = zt, zs, tn, sn
    lane = lax.broadcasted_iota(jnp.int32, (16, LN), 1)
    even = (lane & 1) == 0
    half = lane >> 1
    for i in range(4):
        rr = slice(8 + 16 * i, 24 + 16 * i)
        ro = slice(16 * i, 16 * i + 16)
        tiles = []
        for tile in range(2):
            acc = jnp.zeros((16, LN), F32)
            for f in range(4):
                for l in range(LV):
                    v = pltpu.roll(fa[4 * tile + f, l, rr, :], 2 * l + 1 + 32 * f, 1)
                    acc = jnp.where(half == l + 16 * f, v, acc)
            edge[tile, ro, :] = acc
            tiles.append(acc)
        mr[ro, :] = jnp.where(even, tiles[0], pltpu.roll(tiles[1], 1, 1))
        ml[ro, :] = jnp.where(even, pltpu.roll(tiles[1], LN - 1, 1), tiles[0])
    row = 8 + 63 * c
    for f in range(8):
        for l in range(LV):
            yy[pl.ds(f * LV + l, 1), :] = fa[f, l, pl.ds(row, 1), :]


def face(lo, hi):
    tl, sl_, gtl, gsl, nl, bl, kl, ml = lo
    th, sh, gth, gsh, nh, bh, kh, mh = hi
    ok = jnp.minimum(nl, nh) > 0.0
    db = bh - bl
    slope = jnp.where(ok, -db / (0.5 * (nl + nh) + jnp.abs(db)), 0.0)
    dt = jnp.where(ok, th - tl, 0.0)
    ds = jnp.where(ok, sh - sl_, 0.0)
    a = -0.5 * (kl + kh)
    g = -0.125 * (ml + mh) * slope
    return slope, dt, ds, a * dt + g * (gtl + gth), a * ds + g * (gsl + gsh)


def k2(fa, cs, dep, edge, rl, rr_, yo, yr, msg, cpa, dta, dsa, xf_, xy, yf, car):
    xl, c = place()
    lane = lax.broadcasted_iota(jnp.int32, (16, LN), 1)
    even = (lane & 1) == 0
    first = lane == 0
    last = lane == LN - 1
    for i in range(4):
        ro = slice(16 * i, 16 * i + 16)
        e1, e2, fl, fr = edge[0, ro, :], edge[1, ro, :], rl[ro, :], rr_[ro, :]
        lo1 = jnp.where(even, e1, pltpu.roll(fl, 1, 1))
        lo2 = jnp.where(even, e2, fl)
        hi1 = jnp.where(even, pltpu.roll(fr, LN - 1, 1), e1)
        hi2 = jnp.where(even, fr, e2)
        lo = [pltpu.roll(x, (LN - 32 * q) % LN, 1) if q else x for x in (lo1, lo2) for q in range(4)]
        hi = [pltpu.roll(x, (LN - 32 * q) % LN, 1) if q else x for x in (hi1, hi2) for q in range(4)]
        for q, v in enumerate(face(lo, hi)):
            xf_[q, ro, :] = v
    low = c == 0
    lo, hi = [], []
    for f in range(8):
        a, b = yo[f * LV : f * LV + LV, :], yr[f * LV : f * LV + LV, :]
        lo.append(jnp.where(low, b, a))
        hi.append(jnp.where(low, a, b))
    for q, v in enumerate(face(lo, hi)):
        xy[q] = v
    frow = 7 + 64 * c
    zero = jnp.zeros((RW, LN), F32)
    cpa[0] = zero
    dta[0] = zero
    dsa[0] = zero
    car[5] = zero
    car[6] = zero
    car[7] = zero

    def level(l, close):
        for i in range(3):
            a = 24 * i
            lo = [fa[f, l, a : a + 24, :] for f in range(8)]
            hi = [fa[f, l, a + 1 : a + 25, :] for f in range(8)]
            for q, v in enumerate(face(lo, hi)):
                yf[q, a : a + 24, :] = v
        for q in range(5):
            yf[q, pl.ds(frow, 1), :] = xy[q, pl.ds(l, 1), :]
        kk = l + xl * (32 - 2 * l)
        for i in range(4):
            a = 8 + 16 * i
            ro = slice(16 * i, 16 * i + 16)
            lo = [fa[f, l, a : a + 16, :] for f in range(8)]
            hi = [pltpu.roll(v, LN - 1, 1) for v in lo]
            up, dn = [], []
            for q, v in enumerate(face(lo, hi)):
                b = pltpu.roll(xf_[q, ro, :], LN - 1 - 2 * l, 1)
                up.append(jnp.where(last, b, v))
                dn.append(jnp.where(first, b, pltpu.roll(v, 1, 1)))
            yu = [yf[q, a : a + 16, :] for q in range(5)]
            yd = [yf[q, a - 1 : a + 15, :] for q in range(5)]
            sx, gxt, gxs = (up[q] + dn[q] for q in range(3))
            sy, gyt, gys = (yu[q] + yd[q] for q in range(3))
            ki = lo[6]
            kt = -0.125 * (2.0 * ki - lo[7])
            qt = kt * (sx * gxt + sy * gyt)
            qs = kt * (sx * gxs + sy * gys)
            rh = 0.125 * ki * (sx * sx + sy * sy)
            et = lo[0] - (up[3] - dn[3]) - (yu[3] - yd[3])
            es = lo[1] - (up[4] - dn[4]) - (yu[4] - yd[4])
            if close:
                wz = dep[a : a + 16, :] > kk
                wet = fa[4, l - 1, a : a + 16, :] > 0.0
                ft = jnp.where(wz, car[0, ro, :] + qt, 0.0)
                fs = jnp.where(wz, car[1, ro, :] + qs, 0.0)
                cp = jnp.where(wz, cs[l, a : a + 16, :] + (car[2, ro, :] + rh), 0.0)
                rt = jnp.where(wet, car[3, ro, :] - (ft - car[5, ro, :]), 0.0)
                rs = jnp.where(wet, car[4, ro, :] - (fs - car[6, ro, :]), 0.0)
                up_c = car[7, ro, :]
                inv = 1.0 / (1.0 + cp + up_c * (1.0 - cpa[l - 1, ro, :]))
                cpa[l, ro, :] = cp * inv
                dta[l, ro, :] = (rt + up_c * dta[l - 1, ro, :]) * inv
                dsa[l, ro, :] = (rs + up_c * dsa[l - 1, ro, :]) * inv
                car[5, ro, :] = ft
                car[6, ro, :] = fs
                car[7, ro, :] = cp
            car[0, ro, :] = qt
            car[1, ro, :] = qs
            car[2, ro, :] = rh
            car[3, ro, :] = et
            car[4, ro, :] = es

    level(0, False)

    def step(l, x):
        level(l, True)
        return x

    lax.fori_loop(1, LV, step, 0)
    e = LV - 1
    wet = fa[4, e, 8:72, :] > 0.0
    up_c = car[7]
    msg[0] = car[0]
    msg[1] = car[1]
    msg[2] = cs[LV, 8:72, :] + car[2]
    msg[3] = 1.0 + up_c * (1.0 - cpa[e])
    msg[4] = jnp.where(wet, car[3] + car[5], 0.0) + up_c * dta[e]
    msg[5] = jnp.where(wet, car[4] + car[6], 0.0) + up_c * dsa[e]


def k3(cpa, dta, dsa, dep, me, it, keep, send, xs):
    xl, c = place()
    outer = jnp.where(c == xl, 0, 1)
    for i in range(4):
        ro = slice(16 * i, 16 * i + 16)
        wz = dep[8 + 16 * i : 24 + 16 * i, :] > LV
        cp = jnp.where(wz, me[2, ro, :] + it[2, ro, :], 0.0)
        p, pp = me[3, ro, :], it[3, ro, :]
        inv = 1.0 / (p * pp + cp * (p + pp))
        ww = pp + cp
        v = []
        for q in range(2):
            f = jnp.where(wz, me[q, ro, :] - it[q, ro, :], 0.0)
            v.append((ww * (me[4 + q, ro, :] - f) + cp * (it[4 + q, ro, :] + f)) * inv)
        for l in range(LV - 1, -1, -1):
            if l < LV - 1:
                cc = cpa[l + 1, ro, :]
                v = [dta[l + 1, ro, :] + cc * v[0], dsa[l + 1, ro, :] + cc * v[1]]
            j = l % HB
            j = j + xl * (HB - 1 - 2 * j)
            w = outer if l < HB else 1 - outer
            for q in range(2):
                xs[w, q, j, ro, :] = v[q]
    keep[...] = xs[0]
    send[...] = xs[1]


def k4(keep, got, ot, os_, sem):
    _, c = place()
    mine = pl.multiple_of(RW * c, 8)
    other = pl.multiple_of(RW * (1 - c), 8)
    copies = []
    for q, o in enumerate((ot, os_)):
        copies.append(pltpu.make_async_copy(keep.at[q], o.at[:, pl.ds(mine, RW), :], sem.at[2 * q]))
        copies.append(pltpu.make_async_copy(got.at[q], o.at[:, pl.ds(other, RW), :], sem.at[2 * q + 1]))
    for cp in copies:
        cp.start()
    for cp in copies:
        cp.wait()


def shards(t, s, n, cd, ki, kg, prof, subm):
    nx = lax.axis_size("gx")
    ny = lax.axis_size("gy")
    core = [(0, 1), (1, 0), (2, 3), (3, 2)]
    chip = [(0, 2), (2, 0), (1, 3), (3, 1)]
    cross = [(1, 2), (2, 1), (0, 3), (3, 0)]
    swap, own, al, be = call(
        k0,
        [((6, HB, HW, LN), F32), ((6, HB, HW, LN), F32), ((3, HW, LN), F32), ((3, HW, LN), F32)],
        [HM] * 6,
        [pltpu.SemaphoreType.DMA((12,))],
        name="k0",
    )(t, s, n, ki, kg, cd)
    al = lax.ppermute(al, "gz", cross)
    be = lax.ppermute(be, "gz", chip)
    rec = lax.ppermute(swap, "gz", core)
    fa, cs, dep, edge, mr, ml, yy = call(
        k1,
        [
            ((8, LV, PR, LN), F32),
            ((LV + 1, PR, LN), F32),
            ((PR, LN), jnp.int32),
            ((2, RW, LN), F32),
            ((RW, LN), F32),
            ((RW, LN), F32),
            ((8 * LV, LN), F32),
        ],
        [VM] * 6,
        [pltpu.VMEM((LV, PR, LN), F32)],
        name="k1",
    )(own, rec, al, be, prof, subm)
    east = [(i, (i + 1) % nx) for i in range(nx)]
    west = [(b, a) for a, b in east]
    rows = []
    for y in range(ny - 1):
        for x in range(2):
            a, b = 4 * y + 2 * x + 1, 4 * y + 4 + 2 * x
            rows += [(a, b), (b, a)]
    yr = lax.ppermute(yy, ("gy", "gz"), rows)
    rl = lax.ppermute(mr, "gx", east)
    rr = lax.ppermute(ml, "gx", west)
    msg, cpa, dta, dsa = call(
        k2,
        [((6, RW, LN), F32)] + [((LV, RW, LN), F32)] * 3,
        [VM] * 8,
        [
            pltpu.VMEM((5, RW, LN), F32),
            pltpu.VMEM((5, LV, LN), F32),
            pltpu.VMEM((5, PR, LN), F32),
            pltpu.VMEM((8, RW, LN), F32),
        ],
        name="k2",
    )(fa, cs, dep, edge, rl, rr, yy, yr)
    it = lax.ppermute(msg, "gz", chip)
    keep, send = call(
        k3,
        [((2, HB, RW, LN), F32)] * 2,
        [VM] * 6,
        [pltpu.VMEM((2, 2, HB, RW, LN), F32)],
        name="k3",
    )(cpa, dta, dsa, dep, msg, it)
    got = lax.ppermute(send, "gz", core)
    return tuple(
        call(
            k4,
            [((HB, 2 * RW, LN), F32)] * 2,
            [VM] * 2,
            [pltpu.SemaphoreType.DMA((4,))],
            out_specs=[HM] * 2,
            name="k4",
        )(keep, got)
    )


def solution(mesh):
    block = P("gz", "gy", "gx")
    flat = P("gy", "gx")
    return jax.shard_map(
        shards,
        mesh=mesh,
        in_specs=(block,) * 6 + (flat,) * 2,
        out_specs=(block, block),
        check_vma=False,
    )
```
